16 devices in a mesh: col: 2 (over z), row: 8 (over y, x, core).
Axes of the slice: x: 2, y: 2, z: 2, core: 2. Of those that a mesh axis runs over, the one named last changes fastest.
Arguments:
- vel_u: float32 [41, 1024, 256], P(None, 'row', 'col')
- vel_v: float32 [41, 1024, 256], P(None, 'row', 'col')
- temperature: float32 [41, 1024, 256], P(None, 'row', 'col')
- salinity: float32 [41, 1024, 256], P(None, 'row', 'col')
- sea_level: float32 [1024, 256], P('row', 'col')
- trans_u: float32 [1024, 256], P('row', 'col')
- trans_v: float32 [1024, 256], P('row', 'col')
- col_depth: float32 [1024, 256], P('row', 'col')
- kmt_levels: int32 [1024, 256], P('row', 'col')
Outputs:
- output 1: float32 [1024, 256], P('row', 'col')
- output 2: float32 [1024, 256], P('row', 'col')
- output 3: float32 [1024, 256], P('row', 'col')
- output 4: float32 [41, 1024, 256], P(None, 'row', 'col')
- output 5: float32 [41, 1024, 256], P(None, 'row', 'col')
- output 6: float32 [41, 1024, 256], P(None, 'row', 'col')
- output 7: float32 [41, 1024, 256], P(None, 'row', 'col')
All inputs are finite; a program needn't handle non-finite values.
Results may differ from the reference program's by a relative error of at most 0.001.
Values sent between devices are 32-bit elements.
A program may use at most 1 GiB of HBM per device.

```python
import jax
import jax.numpy as jnp
from jax import lax

LEVELS = 41
GRID_Y = 1024
GRID_X = 256
SUBCYCLES = 30
ADV_COURANT = 0.25
WAVE_COURANT = 0.5
VISC_NUM = 4.0
DIFF_NUM = 1.0
ALPHA_T = 0.3
BETA_S = 0.6


def setup_inputs(seed: int = 0) -> dict:
    sub_keys = jax.random.split(jax.random.key(seed), 12)
    kmt_draw = jax.random.randint(sub_keys[0], (GRID_Y, GRID_X), LEVELS // 3, LEVELS + 1)
    land_draw = jax.random.randint(sub_keys[1], (GRID_Y, GRID_X), 0, 8)
    kmt_levels = jnp.where(land_draw == 0, 0, kmt_draw).astype(jnp.int32)
    kmt_levels = kmt_levels.at[0, 0].set(0).at[0, 1].set(LEVELS)
    col_depth = jax.random.uniform(sub_keys[2], (GRID_Y, GRID_X), jnp.float32, 0.3, 1.0)
    level_frac = jnp.arange(LEVELS, dtype=jnp.float32)[:, None, None] / LEVELS
    shape_3d = (LEVELS, GRID_Y, GRID_X)
    plane_shape = (1, GRID_Y, GRID_X)
    temperature = 1.5 * (1.0 - 2.0 * level_frac) + jax.random.normal(sub_keys[3], plane_shape, jnp.float32) + 0.5 * jax.random.normal(sub_keys[4], shape_3d, jnp.float32)
    salinity = 0.8 * level_frac + 0.8 * jax.random.normal(sub_keys[5], plane_shape, jnp.float32) + 0.4 * jax.random.normal(sub_keys[6], shape_3d, jnp.float32)
    vel_u = 0.5 * jax.random.normal(sub_keys[7], shape_3d, jnp.float32)
    vel_v = 0.5 * jax.random.normal(sub_keys[8], shape_3d, jnp.float32)
    sea_level = 0.5 * jax.random.normal(sub_keys[9], (GRID_Y, GRID_X), jnp.float32)
    trans_u = 0.4 * jax.random.normal(sub_keys[10], (GRID_Y, GRID_X), jnp.float32)
    trans_v = 0.4 * jax.random.normal(sub_keys[11], (GRID_Y, GRID_X), jnp.float32)
    return {'vel_u': vel_u, 'vel_v': vel_v, 'temperature': temperature, 'salinity': salinity, 'sea_level': sea_level, 'trans_u': trans_u, 'trans_v': trans_v, 'col_depth': col_depth, 'kmt_levels': kmt_levels}


def pad_halo(field_in):
    wide_pad = jnp.concatenate([field_in[..., -1:], field_in, field_in[..., :1]], axis=-1)
    zero_row = jnp.zeros_like(wide_pad[..., :1, :])
    return jnp.concatenate([zero_row, wide_pad, zero_row], axis=-2)


def column_solve(wet_mask, diffusivity, rhs_list):
    link_mask = wet_mask[:-1] * wet_mask[1:]
    zero_level = jnp.zeros_like(wet_mask[:1])
    upper_band = diffusivity * jnp.concatenate([link_mask, zero_level], axis=0)
    lower_band = diffusivity * jnp.concatenate([zero_level, link_mask], axis=0)
    diag_band = 1.0 + upper_band + lower_band

    def forward(state_in, level_in):
        c_prev, d_prev = state_in
        up_k, lo_k, dg_k, rhs_k = level_in
        pivot = dg_k - lo_k * c_prev
        c_ratio = up_k / pivot
        d_new = tuple((r + lo_k * p) / pivot for r, p in zip(rhs_k, d_prev))
        return (c_ratio, d_new), (c_ratio, d_new)

    def backward(x_next, level_in):
        c_k, d_k = level_in
        x_new = tuple(d + c_k * x for d, x in zip(d_k, x_next))
        return x_new, x_new

    zero_plane = jnp.zeros_like(wet_mask[0])
    start_state = (zero_plane, tuple(zero_plane for _ in rhs_list))
    _, (c_all, d_all) = lax.scan(forward, start_state, (upper_band, lower_band, diag_band, tuple(rhs_list)))
    _, x_all = lax.scan(backward, tuple(zero_plane for _ in rhs_list), (c_all, d_all), reverse=True)
    return x_all


def upwind_div(u_pad, v_pad, tracer_pad, face_u, face_v):
    u_face = u_pad[:, 1:-1, :-1]
    flux_e = face_u[:, 1:-1, :] * (jnp.maximum(u_face, 0.0) * tracer_pad[:, 1:-1, :-1] + jnp.minimum(u_face, 0.0) * tracer_pad[:, 1:-1, 1:])
    v_face = v_pad[:, :-1, 1:-1]
    flux_n = face_v[:, :, 1:-1] * (jnp.maximum(v_face, 0.0) * tracer_pad[:, :-1, 1:-1] + jnp.minimum(v_face, 0.0) * tracer_pad[:, 1:, 1:-1])
    return flux_e[:, :, 1:] - flux_e[:, :, :-1] + flux_n[:, 1:, :] - flux_n[:, :-1, :]


def baroclinic(u_pad, v_pad, t_pad, s_pad, kmt_pad, depth_pad):
    level_idx = jnp.arange(u_pad.shape[0], dtype=jnp.int32)[:, None, None]
    cell_p = (level_idx < kmt_pad[None]).astype(jnp.float32)
    kmin_u = jnp.minimum(kmt_pad[:, :-1], kmt_pad[:, 1:])
    kmin_v = jnp.minimum(kmt_pad[:-1, :], kmt_pad[1:, :])
    face_u = (level_idx < kmin_u[None]).astype(jnp.float32)
    face_v = (level_idx < kmin_v[None]).astype(jnp.float32)
    thickness = depth_pad / jnp.maximum(kmt_pad, 1).astype(jnp.float32)
    density = (BETA_S * s_pad - ALPHA_T * t_pad) * cell_p
    pressure = (jnp.cumsum(density, axis=0) - 0.5 * density) * thickness[None]
    u_c = u_pad[:, 1:-1, 1:-1]
    v_c = v_pad[:, 1:-1, 1:-1]
    p_c = pressure[:, 1:-1, 1:-1]
    mask_u = face_u[:, 1:-1, 1:]
    mask_v = face_v[:, 1:, 1:-1]
    cell_c = cell_p[:, 1:-1, 1:-1]
    v_at_u = 0.25 * (v_c + v_pad[:, 1:-1, 2:] + v_pad[:, :-2, 1:-1] + v_pad[:, :-2, 2:])
    u_at_v = 0.25 * (u_c + u_pad[:, 1:-1, :-2] + u_pad[:, 2:, 1:-1] + u_pad[:, 2:, :-2])
    tend_u = mask_u * (p_c - pressure[:, 1:-1, 2:] - 0.5 * (u_c * (u_pad[:, 1:-1, 2:] - u_pad[:, 1:-1, :-2]) + v_at_u * (u_pad[:, 2:, 1:-1] - u_pad[:, :-2, 1:-1])))
    tend_v = mask_v * (p_c - pressure[:, 2:, 1:-1] - 0.5 * (u_at_v * (v_pad[:, 1:-1, 2:] - v_pad[:, 1:-1, :-2]) + v_c * (v_pad[:, 2:, 1:-1] - v_pad[:, :-2, 1:-1])))
    new_u = column_solve(mask_u, VISC_NUM, (mask_u * (u_c + ADV_COURANT * tend_u),))[0]
    new_v = column_solve(mask_v, VISC_NUM, (mask_v * (v_c + ADV_COURANT * tend_v),))[0]
    pred_t = cell_c * (t_pad[:, 1:-1, 1:-1] - ADV_COURANT * upwind_div(u_pad, v_pad, t_pad, face_u, face_v))
    pred_s = cell_c * (s_pad[:, 1:-1, 1:-1] - ADV_COURANT * upwind_div(u_pad, v_pad, s_pad, face_u, face_v))
    new_t, new_s = column_solve(cell_c, DIFF_NUM, (pred_t, pred_s))
    count_u = kmin_u[1:-1, 1:]
    count_v = kmin_v[1:, 1:-1]
    wet_u = (count_u > 0).astype(jnp.float32)
    wet_v = (count_v > 0).astype(jnp.float32)
    wet_c = (kmt_pad[1:-1, 1:-1] > 0).astype(jnp.float32)
    inv_u = 1.0 / jnp.maximum(count_u, 1).astype(jnp.float32)
    inv_v = 1.0 / jnp.maximum(count_v, 1).astype(jnp.float32)
    depth_u = 0.5 * (depth_pad[1:-1, 1:-1] + depth_pad[1:-1, 2:]) * wet_u
    depth_v = 0.5 * (depth_pad[1:-1, 1:-1] + depth_pad[2:, 1:-1]) * wet_v
    force_u = depth_u * inv_u * jnp.sum(tend_u, axis=0)
    force_v = depth_v * inv_v * jnp.sum(tend_v, axis=0)
    base_u = new_u - mask_u * (inv_u * jnp.sum(new_u, axis=0))[None]
    base_v = new_v - mask_v * (inv_v * jnp.sum(new_v, axis=0))[None]
    return (base_u, base_v, mask_u, mask_v, new_t, new_s, force_u, force_v, depth_u, depth_v, wet_u, wet_v, wet_c)


def sm_weights():
    frac_step = jnp.arange(1, SUBCYCLES + 1, dtype=jnp.float32) / (SUBCYCLES + 1)
    raw_shape = frac_step ** 2 * (1.0 - frac_step ** 4)
    return raw_shape / jnp.sum(raw_shape)


def barotropic_whole(sea_level, trans_u, trans_v, force_u, force_v, depth_u, depth_v, wet_u, wet_v, wet_c):
    wave_u = WAVE_COURANT * depth_u
    wave_v = WAVE_COURANT * depth_v
    push_u = (ADV_COURANT / SUBCYCLES) * force_u
    push_v = (ADV_COURANT / SUBCYCLES) * force_v

    def subcycle(state_in, weight):
        level_now, flow_u, flow_v, mean_u, mean_v = state_in
        west_u = jnp.roll(flow_u, 1, axis=1)
        south_v = jnp.concatenate([jnp.zeros_like(flow_v[:1]), flow_v[:-1]], axis=0)
        level_new = wet_c * (level_now - WAVE_COURANT * (flow_u - west_u + flow_v - south_v))
        east_level = jnp.roll(level_new, -1, axis=1)
        north_level = jnp.concatenate([level_new[1:], jnp.zeros_like(level_new[:1])], axis=0)
        flow_u = wet_u * (flow_u - wave_u * (east_level - level_new) + push_u)
        flow_v = wet_v * (flow_v - wave_v * (north_level - level_new) + push_v)
        return (level_new, flow_u, flow_v, mean_u + weight * flow_u, mean_v + weight * flow_v), None

    start_state = (wet_c * sea_level, wet_u * trans_u, wet_v * trans_v, jnp.zeros_like(trans_u), jnp.zeros_like(trans_v))
    final_state, _ = lax.scan(subcycle, start_state, sm_weights())
    return final_state


def finish(base_vel, face_mask, mean_flow, face_depth):
    return base_vel + face_mask * (mean_flow / jnp.where(face_depth > 0, face_depth, 1.0))[None]


def reference(vel_u, vel_v, temperature, salinity, sea_level, trans_u, trans_v, col_depth, kmt_levels):
    (base_u, base_v, mask_u, mask_v, new_t, new_s, force_u, force_v, depth_u, depth_v, wet_u, wet_v, wet_c) = baroclinic(pad_halo(vel_u), pad_halo(vel_v), pad_halo(temperature), pad_halo(salinity), pad_halo(kmt_levels), pad_halo(col_depth))
    level_new, flow_u, flow_v, mean_u, mean_v = barotropic_whole(sea_level, trans_u, trans_v, force_u, force_v, depth_u, depth_v, wet_u, wet_v, wet_c)
    return (level_new, flow_u, flow_v, finish(base_u, mask_u, mean_u, depth_u), finish(base_v, mask_v, mean_v, depth_v), new_t, new_s)
```

```python
import functools

import jax
import jax.numpy as jnp
import numpy as np
from jax import lax
from jax.experimental import pallas as pl
from jax.experimental.pallas import tpu as pltpu
from jax.sharding import PartitionSpec as P

SUBCYCLES = 30
ADV_COURANT = 0.25
WAVE_COURANT = 0.5
VISC_NUM = 4.0
DIFF_NUM = 1.0
ALPHA_T = 0.3
BETA_S = 0.6

MESH = pl.DeviceIdType.MESH
f32 = jnp.float32

LV = 41
NB = 128
PAD = 8
NP = NB + 2 * PAD
HW = 32
NW = NB + 2 * HW
NWP = NW + 2 * PAD
R = 32
CH = NB // R
F_STRIDE = 2 * LV
L_KMT = 4 * F_STRIDE
L_DEP = L_KMT + 2


def solver_tables():
    out = np.zeros((8, 128), np.float64)
    for base, a in ((0, VISC_NUM), (3, DIFF_NUM)):
        c = 0.0
        for k in range(LV):
            lo = a if k > 0 else 0.0
            inner = 1.0 / (1.0 + a + lo - lo * c)
            last = 1.0 / (1.0 + lo - lo * c)
            out[base, k] = inner
            out[base + 1, k] = last
            c = a * inner
            out[base + 2, k] = c
    s = np.arange(1, SUBCYCLES + 1) / (SUBCYCLES + 1)
    w = s ** 2 * (1.0 - s ** 4)
    out[6, :SUBCYCLES] = w / w.sum()
    return out.astype(np.float32)


def lanes(rows):
    return lax.broadcasted_iota(jnp.int32, (rows, NB), 1)


def roll(x, s):
    return pltpu.roll(x, s, 1)


def east(x, halo, l0):
    return roll(jnp.where(l0, halo, x), NB - 1)


def west(x, halo, l127):
    return roll(jnp.where(l127, halo, x), 1)


def halo_lanes(ref, lane, rows):
    return roll(ref[lane // NB, rows, :], NB - 1 - lane % NB)


def pack_items(tile):
    items = []
    for f in range(4):
        for k in range(LV):
            lane = f * F_STRIDE + 2 * k
            if lane // NB == tile:
                items.append((f, k, lane % NB))
    return items


def pair(a, b):
    return jnp.where(lanes(a.shape[0]) < 64, roll(a, 32), roll(b, 96))


def unpair(p):
    l = lanes(p.shape[0])
    ok = (l < HW) | (l >= NB - HW)
    return jnp.where(ok, roll(p, 96), 0.0), jnp.where(ok, roll(p, 32), 0.0)


def momentum_kernel(nrow, tab, u_h, v_h, t_h, s_h, eta_r, tu_r, tv_r, dep_r, kmt_r,
                    rowh, pko, kdo, u2, v2, corr, eta_o, tu_o, tv_o,
                    xb, pb, pk, pks, pz, pw, kd, wo, wx, wps, bt, mean,
                    lsem, ssem, rsem):
    col = lax.axis_index("col")
    row = lax.axis_index("row")
    oc = 1 - col
    has_n = row < nrow - 1
    has_s = row > 0

    for f, src in enumerate((u_h, v_h, t_h, s_h)):
        pltpu.make_async_copy(src, xb.at[f, :, pl.ds(PAD, NB), :], lsem.at[f]).start()

    def at_wall(edge, rows, wrows):
        @pl.when(edge)
        def _():
            kd[:, rows, :] = jnp.zeros((2, PAD, NB), f32)
            pk[:, rows, :] = jnp.zeros((3, PAD, NB), f32)
            wo[:, wrows, :] = jnp.zeros((6, HW, NB), f32)
            wx[:, wrows, :] = jnp.zeros((3, HW, NB), f32)

            def zero(k, c):
                for f in range(4):
                    xb[f, k, rows, :] = jnp.zeros((PAD, NB), f32)
                return c
            lax.fori_loop(0, LV, zero, 0)

    at_wall(jnp.logical_not(has_s), pl.ds(0, PAD), pl.ds(0, HW))
    at_wall(jnp.logical_not(has_n), pl.ds(PAD + NB, PAD), pl.ds(HW + NB, HW))

    bar = pltpu.get_barrier_semaphore()

    def greet(dev):
        pl.semaphore_signal(bar, inc=1, device_id=dev, device_id_type=MESH)

    greet({"col": oc, "row": row})

    @pl.when(has_n)
    def _():
        greet({"col": col, "row": row + 1})
        greet({"col": oc, "row": row + 1})

    @pl.when(has_s)
    def _():
        greet({"col": col, "row": row - 1})
        greet({"col": oc, "row": row - 1})

    kmf = kmt_r[...].astype(f32)
    dm = jnp.where(kmt_r[...] > 0, dep_r[...], 0.0)
    kd[0, pl.ds(PAD, NB), :] = kmf
    kd[1, pl.ds(PAD, NB), :] = dm
    own = pl.ds(HW, NB)
    wo[0, own, :] = eta_r[...]
    wo[1, own, :] = tu_r[...]
    wo[2, own, :] = tv_r[...]
    wo[3, own, :] = dm
    wps[0] = pair(eta_r[...], tu_r[...])
    wps[1] = pair(tv_r[...], dm)

    pl.semaphore_wait(bar, 1 + 2 * has_n.astype(jnp.int32) + 2 * has_s.astype(jnp.int32))

    class Group:
        def __init__(self, cond, dev):
            self.cond, self.dev, self.copies = cond, dev, {}

        def add(self, key, sem, src, dst):
            self.copies[key] = pltpu.make_async_remote_copy(
                src_ref=src, dst_ref=dst, send_sem=ssem.at[sem], recv_sem=rsem.at[sem],
                device_id=self.dev, device_id_type=MESH)

        def each(self, keys, what):
            def run():
                for key in keys:
                    what(self.copies[key])
            if self.cond is None:
                run()
            else:
                pl.when(self.cond)(run)

    g_c = Group(None, {"col": oc, "row": row})
    g_n = Group(has_n, {"col": col, "row": row + 1})
    g_s = Group(has_s, {"col": col, "row": row - 1})
    d_n = Group(has_n, {"col": oc, "row": row + 1})
    d_s = Group(has_s, {"col": oc, "row": row - 1})
    hi, lo = pl.ds(PAD + NB - 1, 1), pl.ds(PAD, 1)
    hs, hn = pl.ds(PAD - 1, 1), pl.ds(PAD + NB, 1)
    w_hi, w_lo = pl.ds(NB, HW), pl.ds(HW, HW)
    w_s, w_n = pl.ds(0, HW), pl.ds(HW + NB, HW)
    for t in range(3):
        g_c.add(("p", t), t, pks.at[t], pk.at[t, pl.ds(PAD, NB), :])
    g_c.add("w", 3, wps.at[pl.ds(0, 2)], wx.at[pl.ds(0, 2), own, :])
    g_c.add("f", 4, wps.at[pl.ds(2, 1)], wx.at[pl.ds(2, 1), own, :])
    for f in range(4):
        g_n.add(("x", f), 5 + f, xb.at[f, :, hi, :], xb.at[f, :, hs, :])
        g_s.add(("x", f), 9 + f, xb.at[f, :, lo, :], xb.at[f, :, hn, :])
    g_n.add("k", 13, kd.at[:, hi, :], kd.at[:, hs, :])
    g_s.add("k", 14, kd.at[:, lo, :], kd.at[:, hn, :])
    g_n.add("w", 15, wo.at[pl.ds(0, 4), w_hi, :], wo.at[pl.ds(0, 4), w_s, :])
    g_s.add("w", 16, wo.at[pl.ds(0, 4), w_lo, :], wo.at[pl.ds(0, 4), w_n, :])
    g_n.add("f", 17, wo.at[pl.ds(4, 2), w_hi, :], wo.at[pl.ds(4, 2), w_s, :])
    g_s.add("f", 18, wo.at[pl.ds(4, 2), w_lo, :], wo.at[pl.ds(4, 2), w_n, :])
    d_n.add("p", 19, pks.at[:, pl.ds(NB - 1, 1), :], pk.at[:, hs, :])
    d_s.add("p", 20, pks.at[:, pl.ds(0, 1), :], pk.at[:, hn, :])
    d_n.add("w", 21, wps.at[pl.ds(0, 2), pl.ds(NB - HW, HW), :], wx.at[pl.ds(0, 2), w_s, :])
    d_s.add("w", 22, wps.at[pl.ds(0, 2), pl.ds(0, HW), :], wx.at[pl.ds(0, 2), w_n, :])
    d_n.add("f", 23, wps.at[pl.ds(2, 1), pl.ds(NB - HW, HW), :], wx.at[pl.ds(2, 1), w_s, :])
    d_s.add("f", 24, wps.at[pl.ds(2, 1), pl.ds(0, HW), :], wx.at[pl.ds(2, 1), w_n, :])

    def start(c):
        c.start()

    def wait_send(c):
        c.wait_send()

    def wait_recv(c):
        c.wait_recv()

    g_n.each(["k"], start)
    g_s.each(["k"], start)

    def load_done(f, src):
        pltpu.make_async_copy(src, xb.at[f, :, pl.ds(PAD, NB), :], lsem.at[f]).wait()
        g_n.each([("x", f)], start)
        g_s.each([("x", f)], start)

    def pack_tile(t):
        items = pack_items(t)

        def body(c, carry):
            r = pl.multiple_of(c * R, R)
            rows = pl.ds(pl.multiple_of(c * R + PAD, PAD), R)
            half = lanes(R) // 2
            acc = jnp.zeros((R, NB), f32)
            for f, k, off in items:
                acc = jnp.where(half == off // 2, roll(xb[f, k, rows, :], (off + 1) % NB), acc)
            if t == 2:
                for i, lane in ((0, L_KMT), (1, L_DEP)):
                    off = lane % NB
                    acc = jnp.where(half == off // 2, roll(kd[i, rows, :], (off + 1) % NB), acc)
            pks[t, pl.ds(r, R), :] = acc
            return carry
        lax.fori_loop(0, CH, body, 0)
        g_c.each([("p", t)], start)

    load_done(0, u_h)
    load_done(1, v_h)
    pack_tile(0)
    load_done(2, t_h)
    load_done(3, s_h)
    pack_tile(1)
    pack_tile(2)
    d_n.each(["p"], start)
    d_s.each(["p"], start)
    for g in (g_c, g_n, g_s, d_n, d_s):
        g.each(["w"], start)

    def pressure(r, rows_n):
        rows = pl.ds(r, rows_n)
        km = kd[0, rows, :]
        th = kd[1, rows, :] / jnp.maximum(km, 1.0)

        def level(k, cum):
            rho = jnp.where(k.astype(f32) < km, BETA_S * xb[3, k, rows, :] - ALPHA_T * xb[2, k, rows, :], 0.0)
            new = cum + rho
            pb[k, rows, :] = (new - 0.5 * rho) * th
            return new
        lax.fori_loop(0, LV, level, jnp.zeros((rows_n, NB), f32))

    for c in range(CH):
        pressure(PAD + c * R, R)

    near = [("x", f) for f in range(4)] + ["k"]
    Group_s = Group(has_s, None)
    Group_s.copies = {**g_n.copies, **{("d", k): c for k, c in d_n.copies.items()}}
    Group_n = Group(has_n, None)
    Group_n.copies = {**g_s.copies, **{("d", k): c for k, c in d_s.copies.items()}}
    Group_s.each(near + [("d", "p")], wait_recv)
    Group_n.each(near + [("d", "p")], wait_recv)
    g_c.each([("p", t) for t in range(3)], wait_recv)

    pressure(PAD + NB, PAD)
    mid = pl.ds(PAD, NB)
    pz[0] = pk[0, mid, :] + pk[0, pl.ds(PAD + 1, NB), :]
    pw[0] = pk[0, mid, :] + pk[0, pl.ds(PAD - 1, NB), :]
    pw[1] = pk[1, mid, :] + pk[1, pl.ds(PAD - 1, NB), :]

    def momentum(c):
        r = PAD + c * R
        rows, rows_n, rows_s = pl.ds(r, R), pl.ds(r + 1, R), pl.ds(r - 1, R)
        q = pl.ds(c * R, R)
        lane = lanes(R)
        l0, l127 = lane == 0, lane == NB - 1
        km = kd[0, rows, :]
        dm = kd[1, rows, :]
        hk = halo_lanes(pk, L_KMT, rows)
        hd = halo_lanes(pk, L_DEP, rows)
        hth = hd / jnp.maximum(hk, 1.0)
        nu = jnp.minimum(km, east(km, hk, l0))
        nv = jnp.minimum(km, kd[0, rows_n, :])

        def level(k, carry):
            hc, gus, gvs, du, dv = carry
            kf = k.astype(f32)
            u, un, us = xb[0, k, rows, :], xb[0, k, rows_n, :], xb[0, k, rows_s, :]
            v, vn, vs = xb[1, k, rows, :], xb[1, k, rows_n, :], xb[1, k, rows_s, :]
            hu = halo_lanes(pk, 2 * k, rows)
            hv = halo_lanes(pk, F_STRIDE + 2 * k, rows)
            ht = halo_lanes(pk, 2 * F_STRIDE + 2 * k, rows)
            hs_ = halo_lanes(pk, 3 * F_STRIDE + 2 * k, rows)
            hz = halo_lanes(pz, 2 * k, q)
            hw = halo_lanes(pw, F_STRIDE + 2 * k, q)
            ue, uw = east(u, hu, l0), west(u, hu, l127)
            ve, vw = east(v, hv, l0), west(v, hv, l127)
            w = v + vs
            z = u + un
            w4 = 0.25 * (w + east(w, hw, l0))
            z4 = 0.25 * (z + west(z, hz, l127))
            p, pn = pb[k, rows, :], pb[k, rows_n, :]
            hrho = jnp.where(kf < hk, BETA_S * hs_ - ALPHA_T * ht, 0.0)
            hc = hc + hrho
            pe = east(p, (hc - 0.5 * hrho) * hth, l0)
            gu = p - pe - 0.5 * (u * (ue - uw) + w4 * (un - us))
            gv = p - pn - 0.5 * (z4 * (ve - vw) + v * (vn - vs))
            mu, mv = kf < nu, kf < nv
            gu = jnp.where(mu, gu, 0.0)
            gv = jnp.where(mv, gv, 0.0)
            inner, last = tab[0, k], tab[1, k]
            fu = jnp.where(kf < nu - 1.0, inner, jnp.where(mu, last, 0.0))
            fv = jnp.where(kf < nv - 1.0, inner, jnp.where(mv, last, 0.0))
            du = fu * (u + ADV_COURANT * gu + VISC_NUM * du)
            dv = fv * (v + ADV_COURANT * gv + VISC_NUM * dv)
            u2[k, q, :] = du
            v2[k, q, :] = dv
            return hc, gus + gu, gvs + gv, du, dv

        zero = jnp.zeros((R, NB), f32)
        _, gus, gvs, _, _ = lax.fori_loop(0, LV, level, (zero,) * 5)
        de = east(dm, hd, l0)
        dn = kd[1, rows_n, :]
        hu_ = jnp.where(nu > 0, 0.5 * (dm + de), 0.0)
        hv_ = jnp.where(nv > 0, 0.5 * (dm + dn), 0.0)
        fx = hu_ * gus / jnp.maximum(nu, 1.0)
        fy = hv_ * gvs / jnp.maximum(nv, 1.0)
        wo[4, pl.ds(HW + c * R, R), :] = fx
        wo[5, pl.ds(HW + c * R, R), :] = fy
        wps[2, q, :] = pair(fx, fy)

    for c in range(CH):
        momentum(c)
    for g in (g_c, g_n, g_s, d_n, d_s):
        g.each(["f"], start)

    def back(c):
        r = PAD + c * R
        rows, q = pl.ds(r, R), pl.ds(c * R, R)
        lane = lanes(R)
        km = kd[0, rows, :]
        hk = halo_lanes(pk, L_KMT, rows)
        nu = jnp.minimum(km, east(km, hk, lane == 0))
        nv = jnp.minimum(km, kd[0, pl.ds(r + 1, R), :])

        def level(i, carry):
            xu, xv, su, sv = carry
            k = LV - 1 - i
            ratio = tab[2, k]
            xu = u2[k, q, :] + ratio * xu
            xv = v2[k, q, :] + ratio * xv
            u2[k, q, :] = xu
            v2[k, q, :] = xv
            return xu, xv, su + xu, sv + xv

        zero = jnp.zeros((R, NB), f32)
        _, _, su, sv = lax.fori_loop(0, LV, level, (zero,) * 4)
        mean[0, q, :] = su / jnp.maximum(nu, 1.0)
        mean[1, q, :] = sv / jnp.maximum(nv, 1.0)

    for c in range(CH):
        back(c)

    def halo_rows(k, carry):
        for f in range(4):
            rowh[f, pl.ds(k, 1), :] = xb[f, k, hs, :]
            rowh[4 + f, pl.ds(k, 1), :] = xb[f, k, hn, :]
        return carry
    lax.fori_loop(0, LV, halo_rows, 0)
    pko[...] = pk[:, mid, :]
    kdo[...] = kd[0]

    g_c.each(["w", "f"], wait_recv)
    Group_s.each(["w", "f", ("d", "w"), ("d", "f")], wait_recv)
    Group_n.each(["w", "f", ("d", "w"), ("d", "f")], wait_recv)

    ETA, U, V, WU, WV, PU, PV, WC = range(8)
    for i in range(8):
        for t in range(2):
            for r in (0, PAD + NW):
                bt[i, t, pl.ds(r, PAD), :] = jnp.zeros((PAD, NB), f32)

    def unpack(c, carry):
        src = pl.ds(pl.multiple_of(c * R, R), R)
        dst = pl.ds(pl.multiple_of(c * R + PAD, PAD), R)
        e1, u1 = unpair(wx[0, src, :])
        v1, d1 = unpair(wx[1, src, :])
        x1, y1 = unpair(wx[2, src, :])
        for t, (e, u, v, d, x, y) in enumerate((tuple(wo[i, src, :] for i in range(6)), (e1, u1, v1, d1, x1, y1))):
            bt[ETA, t, dst, :] = e
            bt[U, t, dst, :] = u
            bt[V, t, dst, :] = v
            bt[WC, t, dst, :] = d
            bt[PU, t, dst, :] = (ADV_COURANT / SUBCYCLES) * x
            bt[PV, t, dst, :] = (ADV_COURANT / SUBCYCLES) * y
        return carry
    lax.fori_loop(0, NW // R, unpack, 0)

    wchunks = [PAD + c * R for c in range(NW // R)]
    l0, l127 = lanes(R) == 0, lanes(R) == NB - 1
    for r in wchunks:
        rows = pl.ds(r, R)
        d = [bt[WC, t, rows, :] for t in range(2)]
        dn = [bt[WC, t, pl.ds(r + 1, R), :] for t in range(2)]
        for t in range(2):
            de = east(d[t], d[1 - t], l0)
            fu = (d[t] > 0) & (de > 0)
            fv = (d[t] > 0) & (dn[t] > 0)
            bt[WU, t, rows, :] = jnp.where(fu, WAVE_COURANT * (0.5 * (d[t] + de)), 0.0)
            bt[WV, t, rows, :] = jnp.where(fv, WAVE_COURANT * (0.5 * (d[t] + dn[t])), 0.0)
            bt[U, t, rows, :] = jnp.where(fu, bt[U, t, rows, :], 0.0)
            bt[V, t, rows, :] = jnp.where(fv, bt[V, t, rows, :], 0.0)
            bt[ETA, t, rows, :] = jnp.where(d[t] > 0, bt[ETA, t, rows, :], 0.0)
    for r in wchunks:
        for t in range(2):
            bt[WC, t, pl.ds(r, R), :] = jnp.where(bt[WC, t, pl.ds(r, R), :] > 0, WAVE_COURANT, 0.0)
    corr[...] = jnp.zeros((2, NB, NB), f32)

    def subcycle(n, carry):
        wn = tab[6, n]
        for r in wchunks:
            rows = pl.ds(r, R)
            uu = [bt[U, t, rows, :] for t in range(2)]
            for t in range(2):
                uw = west(uu[t], uu[1 - t], l127)
                div = uu[t] - uw + bt[V, t, rows, :] - bt[V, t, pl.ds(r - 1, R), :]
                bt[ETA, t, rows, :] = bt[ETA, t, rows, :] - bt[WC, t, rows, :] * div
        for i, r in enumerate(wchunks):
            rows = pl.ds(r, R)
            ee = [bt[ETA, t, rows, :] for t in range(2)]
            for t in range(2):
                xe = east(ee[t], ee[1 - t], l0)
                xn = bt[ETA, t, pl.ds(r + 1, R), :]
                un = bt[U, t, rows, :] - bt[WU, t, rows, :] * (xe - ee[t]) + bt[PU, t, rows, :]
                vn = bt[V, t, rows, :] - bt[WV, t, rows, :] * (xn - ee[t]) + bt[PV, t, rows, :]
                bt[U, t, rows, :] = un
                bt[V, t, rows, :] = vn
                if t == 0 and HW + PAD <= r < HW + PAD + NB:
                    q = pl.ds(r - HW - PAD, R)
                    corr[0, q, :] = corr[0, q, :] + wn * un
                    corr[1, q, :] = corr[1, q, :] + wn * vn
        return carry
    lax.fori_loop(0, SUBCYCLES, subcycle, 0)

    core = pl.ds(PAD + HW, NB)
    eta_o[...] = bt[ETA, 0, core, :]
    tu_o[...] = bt[U, 0, core, :]
    tv_o[...] = bt[V, 0, core, :]
    for i, w in ((0, WU), (1, WV)):
        depth = bt[w, 0, core, :] * (1.0 / WAVE_COURANT)
        corr[i] = corr[i] / jnp.where(depth > 0, depth, 1.0) - mean[i]

    g_c.each(list(g_c.copies), wait_send)
    for g in (g_n, g_s, d_n, d_s):
        g.each(list(g.copies), wait_send)


def tracer_kernel(tab, u_h, v_h, t_h, s_h, rowh, pk, kd, u2, v2, corr, eta_r, tu_r, tv_r,
                  eta_o, tu_o, tv_o, uo_h, vo_h, to_h, so_h,
                  xb, out, lsem, osem):
    srcs = (u_h, v_h, t_h, s_h)
    outs = (uo_h, vo_h, to_h, so_h)

    def load(f, c):
        return pltpu.make_async_copy(srcs[f].at[:, pl.ds(c * R, R), :], xb.at[f, :, pl.ds(PAD + c * R, R), :], lsem.at[f, c])

    def store(f, c):
        return pltpu.make_async_copy(out.at[f, :, pl.ds(c * R, R), :], outs[f].at[:, pl.ds(c * R, R), :], osem.at[f, c])

    for c in range(CH):
        for f in range(4):
            load(f, c).start()

    eta_o[...] = eta_r[...]
    tu_o[...] = tu_r[...]
    tv_o[...] = tv_r[...]

    def halo_rows(k, carry):
        for f in range(1, 4):
            xb[f, k, pl.ds(PAD - 1, 1), :] = rowh[f, pl.ds(k, 1), :]
            xb[f, k, pl.ds(PAD + NB, 1), :] = rowh[4 + f, pl.ds(k, 1), :]
        return carry
    lax.fori_loop(0, LV, halo_rows, 0)

    def chunk(c):
        r = PAD + c * R
        rows, rows_n, rows_s = pl.ds(r, R), pl.ds(r + 1, R), pl.ds(r - 1, R)
        q = pl.ds(c * R, R)
        lane = lanes(R)
        l0, l127 = lane == 0, lane == NB - 1
        km = kd[rows, :]
        hk = halo_lanes(pk, L_KMT, q)
        nu = jnp.minimum(km, east(km, hk, l0))
        nuw = jnp.minimum(km, west(km, hk, l127))
        nv = jnp.minimum(km, kd[rows_n, :])
        nvs = jnp.minimum(km, kd[rows_s, :])

        def level(k, carry):
            kf = k.astype(f32)
            u, v, vs = xb[0, k, rows, :], xb[1, k, rows, :], xb[1, k, rows_s, :]
            uw = west(u, halo_lanes(pk, 2 * k, q), l127)
            u = jnp.where(kf < nu, ADV_COURANT * u, 0.0)
            uw = jnp.where(kf < nuw, ADV_COURANT * uw, 0.0)
            v = jnp.where(kf < nv, ADV_COURANT * v, 0.0)
            vs = jnp.where(kf < nvs, ADV_COURANT * vs, 0.0)
            um, vm = jnp.minimum(u, 0.0), jnp.minimum(v, 0.0)
            uwp, vsp = jnp.maximum(uw, 0.0), jnp.maximum(vs, 0.0)
            here = 1.0 - ((u - um) - (uw - uwp) + (v - vm) - (vs - vsp))
            f = jnp.where(kf < km - 1.0, tab[3, k], jnp.where(kf < km, tab[4, k], 0.0))
            new = []
            for i in (2, 3):
                t = xb[i, k, rows, :]
                h = halo_lanes(pk, i * F_STRIDE + 2 * k, q)
                adv = here * t - um * east(t, h, l0) + uwp * west(t, h, l127) - vm * xb[i, k, rows_n, :] + vsp * xb[i, k, rows_s, :]
                d = f * (adv + DIFF_NUM * carry[i - 2])
                out[i, k, q, :] = d
                new.append(d)
            return tuple(new)

        zero = jnp.zeros((R, NB), f32)
        lax.fori_loop(0, LV, level, (zero, zero))
        cu, cv = corr[0, q, :], corr[1, q, :]

        def back(i, carry):
            xt, xs = carry
            k = LV - 1 - i
            kf = k.astype(f32)
            ratio = tab[5, k]
            xt = out[2, k, q, :] + ratio * xt
            xs = out[3, k, q, :] + ratio * xs
            out[2, k, q, :] = xt
            out[3, k, q, :] = xs
            out[0, k, q, :] = u2[k, q, :] + jnp.where(kf < nu, cu, 0.0)
            out[1, k, q, :] = v2[k, q, :] + jnp.where(kf < nv, cv, 0.0)
            return xt, xs
        lax.fori_loop(0, LV, back, (zero, zero))

    for f in range(4):
        load(f, 0).wait()
    for c in range(CH):
        if c + 1 < CH:
            for f in range(4):
                load(f, c + 1).wait()
        chunk(c)
        for f in range(4):
            store(f, c).start()
    for c in range(CH):
        for f in range(4):
            store(f, c).wait()


def solution(mesh):
    nrow = mesh.shape["row"]
    vm = pl.BlockSpec(memory_space=pltpu.VMEM)
    sm = pl.BlockSpec(memory_space=pltpu.SMEM)
    hb = pl.BlockSpec(memory_space=pltpu.HBM)
    table = solver_tables()

    def sds(*shape):
        return jax.ShapeDtypeStruct(shape, f32)

    def step(u, v, t, s, eta, tu, tv, depth, kmt):
        tab = jnp.asarray(table)
        rowh, pk, kd, u2, v2, corr, eta1, tu1, tv1 = pl.pallas_call(
            functools.partial(momentum_kernel, nrow),
            out_shape=(sds(8, LV, NB), sds(3, NB, NB), sds(NP, NB), sds(LV, NB, NB), sds(LV, NB, NB),
                       sds(2, NB, NB), sds(NB, NB), sds(NB, NB), sds(NB, NB)),
            in_specs=[sm] + [hb] * 4 + [vm] * 5,
            out_specs=(vm,) * 9,
            scratch_shapes=[
                pltpu.VMEM((4, LV, NP, NB), f32),
                pltpu.VMEM((LV, NP, NB), f32),
                pltpu.VMEM((3, NP, NB), f32),
                pltpu.VMEM((3, NB, NB), f32),
                pltpu.VMEM((1, NB, NB), f32),
                pltpu.VMEM((2, NB, NB), f32),
                pltpu.VMEM((2, NP, NB), f32),
                pltpu.VMEM((6, NW, NB), f32),
                pltpu.VMEM((3, NW, NB), f32),
                pltpu.VMEM((3, NB, NB), f32),
                pltpu.VMEM((8, 2, NWP, NB), f32),
                pltpu.VMEM((2, NB, NB), f32),
                pltpu.SemaphoreType.DMA((4,)),
                pltpu.SemaphoreType.DMA((25,)),
                pltpu.SemaphoreType.DMA((25,)),
            ],
            compiler_params=pltpu.CompilerParams(collective_id=0, has_side_effects=True, vmem_limit_bytes=34 * 2 ** 20),
            name="momentum",
        )(tab, u, v, t, s, eta, tu, tv, depth, kmt)
        return pl.pallas_call(
            tracer_kernel,
            out_shape=(sds(NB, NB),) * 3 + (sds(LV, NB, NB),) * 4,
            in_specs=[sm] + [hb] * 4 + [vm] * 9,
            out_specs=(vm,) * 3 + (hb,) * 4,
            scratch_shapes=[
                pltpu.VMEM((4, LV, NP, NB), f32),
                pltpu.VMEM((4, LV, NB, NB), f32),
                pltpu.SemaphoreType.DMA((4, CH)),
                pltpu.SemaphoreType.DMA((4, CH)),
            ],
            compiler_params=pltpu.CompilerParams(vmem_limit_bytes=34 * 2 ** 20),
            name="tracers",
        )(tab, u, v, t, s, rowh, pk, kd, u2, v2, corr, eta1, tu1, tv1)

    s3, s2 = P(None, "row", "col"), P("row", "col")
    return jax.shard_map(step, mesh=mesh, in_specs=(s3,) * 4 + (s2,) * 5,
                         out_specs=(s2,) * 3 + (s3,) * 4, check_vma=False)
```

```python
import functools

import jax
import jax.numpy as jnp
import numpy as np
from jax import lax
from jax.experimental import pallas as pl
from jax.experimental.pallas import tpu as pltpu
from jax.sharding import PartitionSpec as P

SUBCYCLES = 30
ADV_COURANT = 0.25
WAVE_COURANT = 0.5
VISC_NUM = 4.0
DIFF_NUM = 1.0
ALPHA_T = 0.3
BETA_S = 0.6

MESH = pl.DeviceIdType.MESH
f32 = jnp.float32

LV = 41
NB = 128
PAD = 8
NP = NB + 2 * PAD
HW = 32
NW = NB + 2 * HW
NWP = NW + 2 * PAD
R = 32
CH = NB // R
L_EXTRA = 2 * LV


def solver_tables():
    out = np.zeros((8, 128), np.float64)
    for base, a in ((0, VISC_NUM), (3, DIFF_NUM)):
        c = 0.0
        for k in range(LV):
            lo = a if k > 0 else 0.0
            inner = 1.0 / (1.0 + a + lo - lo * c)
            last = 1.0 / (1.0 + lo - lo * c)
            out[base, k] = inner
            out[base + 1, k] = last
            c = a * inner
            out[base + 2, k] = c
    s = np.arange(1, SUBCYCLES + 1) / (SUBCYCLES + 1)
    w = s ** 2 * (1.0 - s ** 4)
    out[6, :SUBCYCLES] = w / w.sum()
    return out.astype(np.float32)


def lanes(rows):
    return lax.broadcasted_iota(jnp.int32, (rows, NB), 1)


def roll(x, s):
    return pltpu.roll(x, s, 1)


def east(x, halo, l0):
    return roll(jnp.where(l0, halo, x), NB - 1)


def west(x, halo, l127):
    return roll(jnp.where(l127, halo, x), 1)


def levels(body, init, step):
    def trip(i, carry):
        for j in range(step):
            carry = body(i * step + j, carry)
        return carry
    carry = lax.fori_loop(0, LV // step, trip, init)
    for k in range(LV // step * step, LV):
        carry = body(jnp.int32(k), carry)
    return carry


def pair(a, b):
    return jnp.where(lanes(a.shape[0]) < 64, roll(a, 32), roll(b, 96))


def unpair(p):
    l = lanes(p.shape[0])
    ok = (l < HW) | (l >= NB - HW)
    return jnp.where(ok, roll(p, 96), 0.0), jnp.where(ok, roll(p, 32), 0.0)


def main_kernel(nrow, tab, u_h, v_h, t_h, s_h, eta_r, tu_r, tv_r, dep_r, kmt_r,
                u2, v2, t2, s2, corr, faces, eta_o, tu_o, tv_o,
                xb, sp, sh, pb, cum, hb, pk, pks, pzw, kd, wo, wx, wps, bt, mean,
                lsem, ssem, rsem):
    col = lax.axis_index("col")
    row = lax.axis_index("row")
    oc = 1 - col
    has_n = row < nrow - 1
    has_s = row > 0

    for f, src in enumerate((u_h, v_h, t_h, s_h)):
        pltpu.make_async_copy(src, xb.at[f, :, pl.ds(PAD, NB), :], lsem.at[f]).start()

    def at_wall(edge, rows, wrows):
        @pl.when(edge)
        def _():
            kd[:, rows, :] = jnp.zeros((2, PAD, NB), f32)
            pk[:, rows, :] = jnp.zeros((4, PAD, NB), f32)
            wo[:, wrows, :] = jnp.zeros((6, HW, NB), f32)
            wx[:, wrows, :] = jnp.zeros((3, HW, NB), f32)

            def zero(k, c):
                for f in range(4):
                    xb[f, k, rows, :] = jnp.zeros((PAD, NB), f32)
                return c
            lax.fori_loop(0, LV, zero, 0)

    at_wall(jnp.logical_not(has_s), pl.ds(0, PAD), pl.ds(0, HW))
    at_wall(jnp.logical_not(has_n), pl.ds(PAD + NB, PAD), pl.ds(HW + NB, HW))

    bar = pltpu.get_barrier_semaphore()

    def greet(dev):
        pl.semaphore_signal(bar, inc=1, device_id=dev, device_id_type=MESH)

    greet({"col": oc, "row": row})

    @pl.when(has_n)
    def _():
        greet({"col": col, "row": row + 1})
        greet({"col": oc, "row": row + 1})

    @pl.when(has_s)
    def _():
        greet({"col": col, "row": row - 1})
        greet({"col": oc, "row": row - 1})

    kmf = kmt_r[...].astype(f32)
    dm = jnp.where(kmt_r[...] > 0, dep_r[...], 0.0)
    kd[0, pl.ds(PAD, NB), :] = kmf
    kd[1, pl.ds(PAD, NB), :] = dm
    own = pl.ds(HW, NB)
    wo[0, own, :] = eta_r[...]
    wo[1, own, :] = tu_r[...]
    wo[2, own, :] = tv_r[...]
    wo[3, own, :] = dm
    wps[0] = pair(eta_r[...], tu_r[...])
    wps[1] = pair(tv_r[...], dm)

    pl.semaphore_wait(bar, 1 + 2 * has_n.astype(jnp.int32) + 2 * has_s.astype(jnp.int32))

    class Group:
        def __init__(self, cond, dev):
            self.cond, self.dev, self.copies = cond, dev, {}

        def add(self, key, sem, src, dst):
            self.copies[key] = pltpu.make_async_remote_copy(
                src_ref=src, dst_ref=dst, send_sem=ssem.at[sem], recv_sem=rsem.at[sem],
                device_id=self.dev, device_id_type=MESH)

        def each(self, keys, what):
            def run():
                for key in keys:
                    what(self.copies[key])
            if self.cond is None:
                run()
            else:
                pl.when(self.cond)(run)

    g_c = Group(None, {"col": oc, "row": row})
    g_n = Group(has_n, {"col": col, "row": row + 1})
    g_s = Group(has_s, {"col": col, "row": row - 1})
    d_n = Group(has_n, {"col": oc, "row": row + 1})
    d_s = Group(has_s, {"col": oc, "row": row - 1})
    hi, lo = pl.ds(PAD + NB - 1, 1), pl.ds(PAD, 1)
    hs, hn = pl.ds(PAD - 1, 1), pl.ds(PAD + NB, 1)
    w_hi, w_lo = pl.ds(NB, HW), pl.ds(HW, HW)
    w_s, w_n = pl.ds(0, HW), pl.ds(HW + NB, HW)
    for t in range(4):
        g_c.add(("p", t), 25 + t, pks.at[t], pk.at[t, pl.ds(PAD, NB), :])
    g_c.add("w", 3, wps.at[pl.ds(0, 2)], wx.at[pl.ds(0, 2), own, :])
    g_c.add("f", 4, wps.at[pl.ds(2, 1)], wx.at[pl.ds(2, 1), own, :])
    for f in range(4):
        g_n.add(("x", f), 5 + f, xb.at[f, :, hi, :], xb.at[f, :, hs, :])
        g_s.add(("x", f), 9 + f, xb.at[f, :, lo, :], xb.at[f, :, hn, :])
    g_n.add("k", 13, kd.at[:, hi, :], kd.at[:, hs, :])
    g_s.add("k", 14, kd.at[:, lo, :], kd.at[:, hn, :])
    g_n.add("w", 15, wo.at[pl.ds(0, 4), w_hi, :], wo.at[pl.ds(0, 4), w_s, :])
    g_s.add("w", 16, wo.at[pl.ds(0, 4), w_lo, :], wo.at[pl.ds(0, 4), w_n, :])
    g_n.add("f", 17, wo.at[pl.ds(4, 2), w_hi, :], wo.at[pl.ds(4, 2), w_s, :])
    g_s.add("f", 18, wo.at[pl.ds(4, 2), w_lo, :], wo.at[pl.ds(4, 2), w_n, :])
    d_n.add("p", 19, pks.at[pl.ds(0, 2), pl.ds(NB - 1, 1), :], pk.at[pl.ds(0, 2), hs, :])
    d_s.add("p", 20, pks.at[pl.ds(0, 2), pl.ds(0, 1), :], pk.at[pl.ds(0, 2), hn, :])
    d_n.add("w", 21, wps.at[pl.ds(0, 2), pl.ds(NB - HW, HW), :], wx.at[pl.ds(0, 2), w_s, :])
    d_s.add("w", 22, wps.at[pl.ds(0, 2), pl.ds(0, HW), :], wx.at[pl.ds(0, 2), w_n, :])
    d_n.add("f", 23, wps.at[pl.ds(2, 1), pl.ds(NB - HW, HW), :], wx.at[pl.ds(2, 1), w_s, :])
    d_s.add("f", 24, wps.at[pl.ds(2, 1), pl.ds(0, HW), :], wx.at[pl.ds(2, 1), w_n, :])

    def start(c):
        c.start()

    def wait_send(c):
        c.wait_send()

    def wait_recv(c):
        c.wait_recv()

    g_n.each(["k"], start)
    g_s.each(["k"], start)

    def load_and_pack(f, src):
        pltpu.make_async_copy(src, xb.at[f, :, pl.ds(PAD, NB), :], lsem.at[f]).wait()
        g_n.each([("x", f)], start)
        g_s.each([("x", f)], start)

        def body(c, carry):
            rows = pl.ds(pl.multiple_of(c * R + PAD, PAD), R)
            half = lanes(R) // 2
            acc = jnp.zeros((R, NB), f32)
            for k in range(LV):
                acc = jnp.where(half == k, roll(xb[f, k, rows, :], 2 * k + 1), acc)
            if f < 2:
                acc = jnp.where(half == LV, roll(kd[f, rows, :], L_EXTRA + 1), acc)
            pks[f, pl.ds(pl.multiple_of(c * R, R), R), :] = acc
            return carry
        lax.fori_loop(0, CH, body, 0)
        g_c.each([("p", f)], start)

    load_and_pack(0, u_h)
    load_and_pack(1, v_h)
    d_n.each(["p"], start)
    d_s.each(["p"], start)
    load_and_pack(2, t_h)
    load_and_pack(3, s_h)
    for g in (g_c, g_n, g_s, d_n, d_s):
        g.each(["w"], start)

    mid = pl.ds(PAD, NB)
    cum[...] = jnp.zeros((NB, NB), f32)

    def shift_trip(ks):
        for f in range(4):
            for k in ks:
                for c in range(CH):
                    rows = pl.ds(PAD + c * R, R)
                    x = xb[f, k, rows, :]
                    q = pl.ds(c * R, R)
                    xe, xw = roll(x, NB - 1), roll(x, 1)
                    if f == 0:
                        sh[0, k, q, :] = xe
                        sp[0, k, rows, :] = xw
                    elif f == 1:
                        sp[1, k, rows, :] = xe
                        sh[1, k, q, :] = xw
                    else:
                        sh[2 * f - 2, k, q, :] = xe
                        sh[2 * f - 1, k, q, :] = xw
        for c in range(CH):
            rows, q = pl.ds(PAD + c * R, R), pl.ds(c * R, R)
            depth_of(rows, q, ks)

    def depth_of(rows, q, ks):
        km = kd[0, rows, :]
        th = kd[1, rows, :] / jnp.maximum(km, 1.0)
        total = cum[q, :]
        for k in ks:
            rho = jnp.where(jnp.asarray(k, f32) < km, BETA_S * xb[3, k, rows, :] - ALPHA_T * xb[2, k, rows, :], 0.0)
            new = total + rho
            pb[k, rows, :] = (new - 0.5 * rho) * th
            total = new
        cum[q, :] = total

    def shift_body(i, carry):
        shift_trip([4 * i + j for j in range(4)])
        return carry
    lax.fori_loop(0, LV // 4, shift_body, 0)
    shift_trip([LV - 1])

    near = [("x", f) for f in range(4)] + ["k"]
    from_s = Group(has_s, None)
    from_s.copies = {**g_n.copies, **{("d", k): c for k, c in d_n.copies.items()}}
    from_n = Group(has_n, None)
    from_n.copies = {**g_s.copies, **{("d", k): c for k, c in d_s.copies.items()}}
    from_s.each(near + [("d", "p")], wait_recv)
    from_n.each(near + [("d", "p")], wait_recv)

    below, above = pl.ds(0, PAD), pl.ds(PAD + NB, PAD)
    for k in range(LV):
        sp[0, k, above, :] = roll(xb[0, k, above, :], 1)
        sp[1, k, below, :] = roll(xb[1, k, below, :], NB - 1)
    cum[pl.ds(0, PAD), :] = jnp.zeros((PAD, NB), f32)
    depth_of(above, pl.ds(0, PAD), list(range(LV)))

    g_c.each([("p", t) for t in range(4)], wait_recv)
    odd = lanes(NB) % 2 == 1
    pzw[...] = jnp.where(odd, pk[1, mid, :] + pk[1, pl.ds(PAD - 1, NB), :], pk[0, mid, :] + pk[0, pl.ds(PAD + 1, NB), :])

    def columns(c):
        r = PAD + c * R
        rows, rows_n, rows_s = pl.ds(r, R), pl.ds(r + 1, R), pl.ds(r - 1, R)
        q = pl.ds(c * R, R)
        lane = lanes(R)
        l0, l127 = lane == 0, lane == NB - 1

        def packed(f):
            return pzw[q, :] if f == 4 else pk[f, rows, :]

        def edge_east(f, x):
            return jnp.where(l127, roll(pk[f, rows, :], NB - 2 - L_EXTRA), roll(x, NB - 1))

        km = kd[0, rows, :]
        dm = kd[1, rows, :]
        ke, de = edge_east(0, km), edge_east(1, dm)
        kw = jnp.where(l0, roll(pk[0, rows, :], NB - L_EXTRA), roll(km, 1))
        the = de / jnp.maximum(ke, 1.0)
        nu = jnp.minimum(km, ke)
        nuw = jnp.minimum(km, kw)
        nv = jnp.minimum(km, kd[0, rows_n, :])
        nvs = jnp.minimum(km, kd[0, rows_s, :])
        faces[0, q, :] = nu
        faces[1, q, :] = nv

        for f in range(5):
            hb[0, f] = packed(f)
            hb[1, f] = roll(packed(f), NB - 2)

        def level(k, carry):
            ce, gus, gvs, du, dv, dt, ds = carry
            kf = k.astype(f32)
            kf1 = kf + 1.0
            u, un, us = xb[0, k, rows, :], xb[0, k, rows_n, :], xb[0, k, rows_s, :]
            v, vn, vs = xb[1, k, rows, :], xb[1, k, rows_n, :], xb[1, k, rows_s, :]

            slot_e, slot_w, slot_new = lax.rem(k + 1, 4), lax.rem(k, 4), lax.rem(k + 2, 4)

            def he(f, x):
                return jnp.where(l127, hb[slot_e, f], x)

            def hw(f, x):
                return jnp.where(l0, hb[slot_w, f], x)

            ue, uw = sh[0, k, q, :], sp[0, k, rows, :]
            ve, vw = sp[1, k, rows, :], sh[1, k, q, :]
            wsum = v + vs + he(4, ve + sp[1, k, rows_s, :])
            zsum = u + un + hw(4, uw + sp[0, k, rows_n, :])
            ue, uw, ve, vw = he(0, ue), hw(0, uw), he(1, ve), hw(1, vw)
            t, s = xb[2, k, rows, :], xb[3, k, rows, :]
            te, tw = he(2, sh[2, k, q, :]), hw(2, sh[3, k, q, :])
            se, sw = he(3, sh[4, k, q, :]), hw(3, sh[5, k, q, :])
            rho = jnp.where(kf < ke, BETA_S * se - ALPHA_T * te, 0.0)
            ce = ce + rho
            p = pb[k, rows, :]
            gu = p - (ce - 0.5 * rho) * the - (0.5 * u * (ue - uw) + (0.125 * wsum) * (un - us))
            gv = p - pb[k, rows_n, :] - ((0.125 * zsum) * (ve - vw) + 0.5 * v * (vn - vs))
            mu, mv = kf < nu, kf < nv
            gu = jnp.where(mu, gu, 0.0)
            gv = jnp.where(mv, gv, 0.0)
            inner, last = tab[0, k], tab[1, k]
            fu = jnp.where(kf1 < nu, inner, jnp.where(mu, last, 0.0))
            fv = jnp.where(kf1 < nv, inner, jnp.where(mv, last, 0.0))
            du = fu * (u + ADV_COURANT * gu + VISC_NUM * du)
            dv = fv * (v + ADV_COURANT * gv + VISC_NUM * dv)
            u2[k, q, :] = du
            v2[k, q, :] = dv
            u = jnp.where(mu, ADV_COURANT * u, 0.0)
            v = jnp.where(mv, ADV_COURANT * v, 0.0)
            uw = jnp.where(kf < nuw, ADV_COURANT * uw, 0.0)
            vs = jnp.where(kf < nvs, ADV_COURANT * vs, 0.0)
            um, vm = jnp.minimum(u, 0.0), jnp.minimum(v, 0.0)
            uwp, vsp = jnp.maximum(uw, 0.0), jnp.maximum(vs, 0.0)
            here = 1.0 - (((u - um) - (uw - uwp)) + ((v - vm) - (vs - vsp)))
            fc = jnp.where(kf1 < km, tab[3, k], jnp.where(kf < km, tab[4, k], 0.0))

            def tracer(i, x, xe, xw, d):
                moved = here * x + (uwp * xw - um * xe) + (vsp * xb[i, k, rows_s, :] - vm * xb[i, k, rows_n, :])
                return fc * (moved + DIFF_NUM * d)

            dt = tracer(2, t, te, tw, dt)
            ds = tracer(3, s, se, sw, ds)
            t2[k, q, :] = dt
            s2[k, q, :] = ds
            for f in range(5):
                hb[slot_new, f] = roll(packed(f), NB - 4 - 2 * k)
            return ce, gus + gu, gvs + gv, du, dv, dt, ds

        zero = jnp.zeros((R, NB), f32)
        _, gus, gvs, _, _, _, _ = levels(level, (zero,) * 7, 1)
        dn = kd[1, rows_n, :]
        hu = jnp.where(nu > 0, 0.5 * (dm + de), 0.0)
        hv = jnp.where(nv > 0, 0.5 * (dm + dn), 0.0)
        fx = hu * gus / jnp.maximum(nu, 1.0)
        fy = hv * gvs / jnp.maximum(nv, 1.0)
        wo[4, pl.ds(HW + c * R, R), :] = fx
        wo[5, pl.ds(HW + c * R, R), :] = fy
        wps[2, q, :] = pair(fx, fy)

    for c in range(CH):
        columns(c)
    for g in (g_c, g_n, g_s, d_n, d_s):
        g.each(["f"], start)

    def back(c):
        q = pl.ds(c * R, R)

        def level(i, carry):
            xu, xv, xt, xs, su, sv = carry
            k = LV - 1 - i
            ru, rc = tab[2, k], tab[5, k]
            xu = u2[k, q, :] + ru * xu
            xv = v2[k, q, :] + ru * xv
            xt = t2[k, q, :] + rc * xt
            xs = s2[k, q, :] + rc * xs
            u2[k, q, :] = xu
            v2[k, q, :] = xv
            t2[k, q, :] = xt
            s2[k, q, :] = xs
            return xu, xv, xt, xs, su + xu, sv + xv

        zero = jnp.zeros((R, NB), f32)
        out = levels(level, (zero,) * 6, 4)
        mean[0, q, :] = out[4] / jnp.maximum(faces[0, q, :], 1.0)
        mean[1, q, :] = out[5] / jnp.maximum(faces[1, q, :], 1.0)

    for c in range(CH):
        back(c)

    g_c.each(["w", "f"], wait_recv)
    from_s.each(["w", "f", ("d", "w"), ("d", "f")], wait_recv)
    from_n.each(["w", "f", ("d", "w"), ("d", "f")], wait_recv)

    ETA, U, V, WU, WV, PU, PV, WC = range(8)
    for i in range(8):
        for t in range(2):
            for r in (0, PAD + NW):
                bt[i, t, pl.ds(r, PAD), :] = jnp.zeros((PAD, NB), f32)

    def unpack(c, carry):
        src = pl.ds(pl.multiple_of(c * R, R), R)
        dst = pl.ds(pl.multiple_of(c * R + PAD, PAD), R)
        e1, u1 = unpair(wx[0, src, :])
        v1, d1 = unpair(wx[1, src, :])
        x1, y1 = unpair(wx[2, src, :])
        for t, (e, u, v, d, x, y) in enumerate((tuple(wo[i, src, :] for i in range(6)), (e1, u1, v1, d1, x1, y1))):
            bt[ETA, t, dst, :] = e
            bt[U, t, dst, :] = u
            bt[V, t, dst, :] = v
            bt[WC, t, dst, :] = d
            bt[PU, t, dst, :] = (ADV_COURANT / SUBCYCLES) * x
            bt[PV, t, dst, :] = (ADV_COURANT / SUBCYCLES) * y
        return carry
    lax.fori_loop(0, NW // R, unpack, 0)

    wchunks = [PAD + c * R for c in range(NW // R)]
    l0, l127 = lanes(R) == 0, lanes(R) == NB - 1
    for r in wchunks:
        rows = pl.ds(r, R)
        d = [bt[WC, t, rows, :] for t in range(2)]
        dn = [bt[WC, t, pl.ds(r + 1, R), :] for t in range(2)]
        for t in range(2):
            de = east(d[t], d[1 - t], l0)
            fu = (d[t] > 0) & (de > 0)
            fv = (d[t] > 0) & (dn[t] > 0)
            bt[WU, t, rows, :] = jnp.where(fu, WAVE_COURANT * (0.5 * (d[t] + de)), 0.0)
            bt[WV, t, rows, :] = jnp.where(fv, WAVE_COURANT * (0.5 * (d[t] + dn[t])), 0.0)
            bt[U, t, rows, :] = jnp.where(fu, bt[U, t, rows, :], 0.0)
            bt[V, t, rows, :] = jnp.where(fv, bt[V, t, rows, :], 0.0)
            bt[ETA, t, rows, :] = jnp.where(d[t] > 0, bt[ETA, t, rows, :], 0.0)
    for r in wchunks:
        for t in range(2):
            bt[WC, t, pl.ds(r, R), :] = jnp.where(bt[WC, t, pl.ds(r, R), :] > 0, WAVE_COURANT, 0.0)
    corr[...] = jnp.zeros((2, NB, NB), f32)

    def subcycle(n, carry):
        wn = tab[6, n]
        for r in wchunks:
            rows = pl.ds(r, R)
            uu = [bt[U, t, rows, :] for t in range(2)]
            for t in range(2):
                uw = west(uu[t], uu[1 - t], l127)
                div = uu[t] - uw + bt[V, t, rows, :] - bt[V, t, pl.ds(r - 1, R), :]
                bt[ETA, t, rows, :] = bt[ETA, t, rows, :] - bt[WC, t, rows, :] * div
        for i, r in enumerate(wchunks):
            rows = pl.ds(r, R)
            ee = [bt[ETA, t, rows, :] for t in range(2)]
            for t in range(2):
                xe = east(ee[t], ee[1 - t], l0)
                xn = bt[ETA, t, pl.ds(r + 1, R), :]
                un = bt[U, t, rows, :] - bt[WU, t, rows, :] * (xe - ee[t]) + bt[PU, t, rows, :]
                vn = bt[V, t, rows, :] - bt[WV, t, rows, :] * (xn - ee[t]) + bt[PV, t, rows, :]
                bt[U, t, rows, :] = un
                bt[V, t, rows, :] = vn
                if t == 0 and HW + PAD <= r < HW + PAD + NB:
                    q = pl.ds(r - HW - PAD, R)
                    corr[0, q, :] = corr[0, q, :] + wn * un
                    corr[1, q, :] = corr[1, q, :] + wn * vn
        return carry
    lax.fori_loop(0, SUBCYCLES, subcycle, 0)

    core = pl.ds(PAD + HW, NB)
    eta_o[...] = bt[ETA, 0, core, :]
    tu_o[...] = bt[U, 0, core, :]
    tv_o[...] = bt[V, 0, core, :]
    for i, w in ((0, WU), (1, WV)):
        depth = bt[w, 0, core, :] * (1.0 / WAVE_COURANT)
        corr[i] = corr[i] / jnp.where(depth > 0, depth, 1.0) - mean[i]

    g_c.each(list(g_c.copies), wait_send)
    for g in (g_n, g_s, d_n, d_s):
        g.each(list(g.copies), wait_send)


def finish_kernel(u2, v2, t2, s2, corr, faces, eta_r, tu_r, tv_r,
                  eta_o, tu_o, tv_o, uo_h, vo_h, to_h, so_h, out, tsem, osem):
    tracers = [pltpu.make_async_copy(src, dst, tsem.at[i]) for i, (src, dst) in enumerate(((t2, to_h), (s2, so_h)))]
    for copy in tracers:
        copy.start()
    eta_o[...] = eta_r[...]
    tu_o[...] = tu_r[...]
    tv_o[...] = tv_r[...]
    copies = []
    for c in range(CH):
        q = pl.ds(c * R, R)
        for i, (src, dst) in enumerate(((u2, uo_h), (v2, vo_h))):
            n, add = faces[i, q, :], corr[i, q, :]

            def level(k, carry):
                out[i, k, q, :] = src[k, q, :] + jnp.where(k.astype(f32) < n, add, 0.0)
                return carry
            levels(level, 0, 8)
            copy = pltpu.make_async_copy(out.at[i, :, q, :], dst.at[:, q, :], osem.at[i, c])
            copy.start()
            copies.append(copy)
    for copy in tracers + copies:
        copy.wait()


def solution(mesh):
    nrow = mesh.shape["row"]
    vm = pl.BlockSpec(memory_space=pltpu.VMEM)
    sm = pl.BlockSpec(memory_space=pltpu.SMEM)
    hb = pl.BlockSpec(memory_space=pltpu.HBM)
    table = solver_tables()

    def sds(*shape):
        return jax.ShapeDtypeStruct(shape, f32)

    def step(*args):
        args = [pltpu.with_memory_space_constraint(x, pltpu.HBM) for x in (jnp.asarray(table),) + args]
        outs = pl.pallas_call(
            functools.partial(main_kernel, nrow),
            out_shape=(sds(LV, NB, NB),) * 4 + (sds(2, NB, NB),) * 2 + (sds(NB, NB),) * 3,
            in_specs=[sm] + [hb] * 4 + [vm] * 5,
            out_specs=(vm,) * 9,
            scratch_shapes=[
                pltpu.VMEM((4, LV, NP, NB), f32),
                pltpu.VMEM((2, LV, NP, NB), f32),
                pltpu.VMEM((6, LV, NB, NB), f32),
                pltpu.VMEM((LV, NP, NB), f32),
                pltpu.VMEM((NB, NB), f32),
                pltpu.VMEM((4, 5, R, NB), f32),
                pltpu.VMEM((4, NP, NB), f32),
                pltpu.VMEM((4, NB, NB), f32),
                pltpu.VMEM((NB, NB), f32),
                pltpu.VMEM((2, NP, NB), f32),
                pltpu.VMEM((6, NW, NB), f32),
                pltpu.VMEM((3, NW, NB), f32),
                pltpu.VMEM((3, NB, NB), f32),
                pltpu.VMEM((8, 2, NWP, NB), f32),
                pltpu.VMEM((2, NB, NB), f32),
                pltpu.SemaphoreType.DMA((4,)),
                pltpu.SemaphoreType.DMA((29,)),
                pltpu.SemaphoreType.DMA((29,)),
            ],
            compiler_params=pltpu.CompilerParams(collective_id=0, has_side_effects=True, vmem_limit_bytes=41 * 2 ** 20),
            name="ocean",
        )(*args)
        return pl.pallas_call(
            finish_kernel,
            out_shape=(sds(NB, NB),) * 3 + (sds(LV, NB, NB),) * 4,
            in_specs=[vm] * 9,
            out_specs=(vm,) * 3 + (hb,) * 4,
            scratch_shapes=[
                pltpu.VMEM((2, LV, NB, NB), f32),
                pltpu.SemaphoreType.DMA((2,)),
                pltpu.SemaphoreType.DMA((2, CH)),
            ],
            compiler_params=pltpu.CompilerParams(vmem_limit_bytes=12 * 2 ** 20),
            name="finish",
        )(*outs)

    s3, s2 = P(None, "row", "col"), P("row", "col")
    return jax.shard_map(step, mesh=mesh, in_specs=(s3,) * 4 + (s2,) * 5,
                         out_specs=(s2,) * 3 + (s3,) * 4, check_vma=False)
```
